32 devices in a mesh: dp: 8 (over z, x), mp: 4 (over y, core).
Axes of the slice: x: 2, y: 2, z: 4, core: 2. Of those that a mesh axis runs over, the one named last changes fastest.
Arguments:
- gradients: bfloat16 [8, 2, 4096, 1024], P('dp', None, None, 'mp'), may hold values from -6912 to 6912
- layer_mask: int32 [8, 2], P('dp'), may hold values from 0 to 1, as said below
- exit_losses: float32 [8, 2], P('dp'), may hold values from 1 to 24
- exit_weights: int32 [2], replicated, may hold values from 1 to 8
- params: float32 [2, 4096, 1024], P(None, 'dp', 'mp'), may hold values from -0.3 to 0.3
- moment: float32 [2, 4096, 1024], P(None, 'dp', 'mp'), may hold values from -6 to 6
- second: float32 [2, 4096, 1024], P(None, 'dp', 'mp'), may hold values from 0.5 to 4
Outputs:
- new_params: float32 [2, 4096, 1024], P(None, 'dp', 'mp')
- new_moment: float32 [2, 4096, 1024], P(None, 'dp', 'mp')
- new_second: float32 [2, 4096, 1024], P(None, 'dp', 'mp')
- exit_mean: float32 [2], replicated
The draws below stay inside these ranges and needn't reach their ends.
Inputs may be any that keep to these rules, and one draw needn't show every extreme that they name: `layer_mask`: every layer is run by at least one micro-batch.
All inputs are finite; a program needn't handle non-finite values.
Results may differ from the reference program's by a relative error of at most 0.0003.
Values sent between devices are 32-bit elements; how exact they have to be, the bound alone decides.
A program may use at most 64 MiB of HBM per device.

```python
import math
import jax
import jax.numpy as jnp
from jax import lax

D = 4096
KVW = 1024
LAYERS = 2
MB = 8


def draw_gradients(key, part):
    key_rows = jax.random.fold_in(key, 0)
    key_cols = jax.random.fold_in(key, 1)
    key_noise = jax.random.fold_in(key, 3)
    row_scale = jnp.exp(jax.random.uniform(key_rows, (D,), jnp.float32, math.log(0.3), math.log(3.0)))
    col_scale = jnp.exp(jax.random.uniform(key_cols, (KVW,), jnp.float32, math.log(0.3), math.log(3.0)))
    values = jax.random.normal(key_noise, (MB, LAYERS, D, KVW), jnp.float32)
    values = jnp.clip(values, -6.0, 6.0) * 128.0 * row_scale[:, None] * col_scale[None, :]
    return values.astype(jnp.bfloat16)


def draw_layer_mask(key, part):
    key_keep, key_force = jax.random.split(key)
    raw_draws = jax.random.randint(key_keep, (MB, LAYERS), 0, 1000)
    depth_index = jnp.arange(LAYERS, dtype=jnp.int32)
    threshold = 900 - 400 * depth_index // max(LAYERS - 1, 1)
    keep_flag = (raw_draws < threshold[None, :]).astype(jnp.int32)
    forced = jax.random.randint(key_force, (LAYERS,), 0, MB)
    row_index = jnp.arange(MB, dtype=jnp.int32)
    chosen = (row_index[:, None] == forced[None, :]).astype(jnp.int32)
    return jnp.maximum(keep_flag, chosen)


def draw_exit_losses(key, part):
    ramp = 1.0 + 2.0 * jnp.arange(MB, dtype=jnp.float32) / max(MB - 1, 1)
    base = jnp.exp(jax.random.uniform(key, (MB, LAYERS), jnp.float32, math.log(1.5), math.log(4.0)))
    return (ramp[:, None] * base).astype(jnp.float32)


def steps_of(stream_key, dims, cuts, smallest, high):
    level = 1.0
    for position, shards_of in cuts:
        heights = jax.random.uniform(jax.random.fold_in(jax.random.fold_in(stream_key, 6), position), (shards_of,), jnp.float32, smallest / len(cuts), high / len(cuts))
        level = level * jnp.repeat(jnp.exp(heights), dims[position] // shards_of).reshape((-1,) + (1,) * (len(dims) - 1 - position))
    return level


def gaussian(key, extent, scale, reach, shards=(), held_as=jnp.bfloat16):
    entries = scale * jax.random.normal(key, extent, jnp.float32)
    if shards:
        entries = entries * steps_of(key, extent, shards, -0.22, 0.18)
    return jnp.clip(entries, -reach, reach).astype(held_as)


def setup_inputs(seed: int = 0) -> dict:
    keys = jax.random.split(jax.random.key(seed), 8)
    gradients = draw_gradients(jax.random.fold_in(keys[7], 71), 0)
    layer_mask = draw_layer_mask(jax.random.fold_in(keys[7], 71), 0)
    exit_losses = draw_exit_losses(jax.random.fold_in(keys[7], 71), 0)
    exit_weights = jax.random.randint(keys[3], (LAYERS,), 1, 9).astype(jnp.int32)
    params = gaussian(keys[4], (LAYERS, D, KVW), 0.05, 0.3, ((1, 8), (2, 4)), jnp.float32)
    moment = gaussian(keys[5], (LAYERS, D, KVW), 1.0, 6.0, ((1, 8), (2, 4)), jnp.float32)
    second = jnp.clip(jnp.exp(math.log(4.0) - 2.0794415 * jax.random.uniform(keys[6], (LAYERS, D, KVW), jnp.float32) ** steps_of(keys[6], (LAYERS, D, KVW), ((1, 8), (2, 4)), -0.2, 0.2)), 0.5, 4.0)
    return dict(gradients=gradients, layer_mask=layer_mask, exit_losses=exit_losses, exit_weights=exit_weights, params=params, moment=moment, second=second)


max_rms = 1.0
eps_norm = 1e-06
eps_adam = 1e-08
beta_one = 0.9
beta_two = 0.95
learn_rate = 0.01
decay_rate = 0.1

def reference(gradients, layer_mask, exit_losses, exit_weights, params, moment, second):
    keep_float = layer_mask.astype(jnp.float32)
    layer_count = lax.optimization_barrier(jnp.sum(keep_float, axis=0))
    exit_mean = lax.optimization_barrier(jnp.sum(keep_float * exit_losses, axis=0)) / layer_count
    weight_float = exit_weights.astype(jnp.float32)
    weight_sum = jnp.sum(weight_float)

    def accumulate(running, pieces):
        block, keep_row = pieces
        return (running + block.astype(jnp.float32) * keep_row[:, None, None], None)
    summed, unused = lax.scan(accumulate, jnp.zeros((LAYERS, D, KVW), jnp.float32), (gradients, keep_float))
    factor_row = weight_float / (weight_sum * layer_count)
    gradient = summed * factor_row[:, None, None]
    rms_value = jnp.sqrt(jnp.sum(gradient * gradient) / (LAYERS * D * KVW))
    clip_scale = jnp.minimum(1.0, max_rms / (rms_value + eps_norm))
    clipped = clip_scale * gradient
    new_moment = beta_one * moment + (1.0 - beta_one) * clipped
    new_second = beta_two * second + (1.0 - beta_two) * clipped * clipped
    new_params = params - learn_rate * (new_moment / (jnp.sqrt(new_second) + eps_adam) + decay_rate * params)
    return (new_params, new_moment, new_second, exit_mean)
```

```python
import jax
import jax.numpy as jnp
from jax import lax
from jax.experimental import pallas as pl
from jax.experimental.pallas import tpu as pltpu
from jax.sharding import PartitionSpec as P

max_rms = 1.0
eps_norm = 1e-06
eps_adam = 1e-08
beta_one = 0.9
beta_two = 0.95
learn_rate = 0.01
decay_rate = 0.1

MESH_ID = pl.DeviceIdType.MESH
ROWS = 128
LAG = 2
MINE, OTHER = 0, 1


def update(gradient, square_sum, entries, params, moment, second):
    rms_value = jnp.sqrt(square_sum / entries)
    clip_scale = jnp.minimum(1.0, max_rms / (rms_value + eps_norm))
    clipped = clip_scale * gradient
    new_moment = beta_one * moment + (1.0 - beta_one) * clipped
    new_second = beta_two * second + (1.0 - beta_two) * clipped * clipped
    new_params = params - learn_rate * (
        new_moment / (jnp.sqrt(new_second) + eps_adam) + decay_rate * params
    )
    return new_params, new_moment, new_second


def any_mesh_body(entries, gradients, layer_mask, exit_losses, exit_weights, params, moment, second):
    keep_float = layer_mask[0].astype(jnp.float32)
    loss_terms = keep_float * exit_losses[0]
    local_term = gradients[0].astype(jnp.float32) * keep_float[:, None, None]
    summed = lax.psum_scatter(local_term, "dp", scatter_dimension=1, tiled=True)
    weight_float = exit_weights.astype(jnp.float32)
    weight_sum = jnp.sum(weight_float)
    layer_count, loss_sum = lax.psum((keep_float, loss_terms), "dp")
    gradient = summed * (weight_float / (weight_sum * layer_count))[:, None, None]
    square_sum = lax.psum(jnp.sum(gradient * gradient), ("dp", "mp"))
    new = update(gradient, square_sum, entries, params, moment, second)
    return (*new, loss_sum / layer_count)


def line_kernel(
    n_mp, mask, losses, weights, grads, out, stats_out, square_out,
    held, snd, xr, zr, ar, st0, st1, st2, square,
    load_sem, send_sem, x_sem, z_sem, a_sem,
    st0_send, st0_recv, st1_send, st1_recv, st2_send, st2_recv,
):
    layers, rows = out.shape[0], out.shape[1]
    pieces = snd.shape[1]
    depth = snd.shape[2]
    per_layer = pieces // layers
    early = pieces // 2
    dp, mp = lax.axis_index("dp"), lax.axis_index("mp")
    z, x = dp // 2, lax.rem(dp, 2)
    upper = z // 2
    place = lax.rem(z + upper, 2)
    x_dev = z * 2 + 1 - x
    z_dev = (z + 1 - 2 * lax.rem(z, 2)) * 2 + x
    a_dev = (3 - z) * 2 + x

    def load(slot, layer):
        k, side = slot // 2, slot % 2
        target = (k + upper * (3 - 2 * k)) * 2 + (x if side == MINE else 1 - x)
        return pltpu.make_async_copy(
            grads.at[0, layer, pl.ds(target * rows, rows), :], held.at[slot, layer], load_sem.at[slot, layer]
        )

    order = (7, 3, 1, 6, 5, 4, 2, 0)
    for slot in order:
        for layer in range(layers):
            load(slot, layer).start()

    def loaded(*slots):
        for slot in slots:
            for layer in range(layers):
                load(slot, layer).wait()

    row = lax.broadcasted_iota(jnp.int32, st0.shape[1:], 0)
    tile = jnp.zeros(st0.shape[1:], jnp.float32)
    for layer in range(layers):
        keep = mask[0, layer].astype(jnp.float32)
        tile = jnp.where(row == layer, keep, tile)
        tile = jnp.where(row == layers + layer, keep * losses[0, layer], tile)
    st0[dp] = tile

    barrier = pltpu.get_barrier_semaphore()
    for i in range(1, 8):
        pl.semaphore_signal(barrier, inc=1, device_id={"dp": lax.rem(dp + i, 8)}, device_id_type=MESH_ID)
    for i in range(1, n_mp):
        for xx in (x, 1 - x):
            pl.semaphore_signal(
                barrier, inc=1, device_id={"dp": z * 2 + xx, "mp": lax.rem(mp + i, n_mp)}, device_id_type=MESH_ID
            )
    pl.semaphore_wait(barrier, 7 + 2 * (n_mp - 1))

    def own(slot, c):
        layer, r = c // per_layer, lax.rem(c, per_layer)
        keep = mask[0, layer].astype(jnp.float32)
        return held[slot, layer, pl.ds(pl.multiple_of(r * depth, depth), depth), :].astype(jnp.float32) * keep

    def push(slot, c, dst, sem, device):
        return pltpu.make_async_remote_copy(
            src_ref=snd.at[slot, c], dst_ref=dst, send_sem=send_sem.at[slot, c], recv_sem=sem,
            device_id={"dp": device}, device_id_type=MESH_ID,
        )

    def to_x(k, c):
        return push(2 * k + OTHER, c, xr.at[k, c], x_sem.at[k, c], x_dev)

    def to_z(slot, box, c):
        return push(slot, c, zr.at[box, c], z_sem.at[box, c], z_dev)

    def to_a(k, c):
        return push(2 * k + MINE, c, ar.at[3 - k, c], a_sem.at[3 - k, c], a_dev)

    def from_x(k, c):
        to_x(k, c).wait_recv()
        return xr[k, c]

    def from_z(box, c):
        to_z(0, box, c).wait_recv()
        return zr[box, c]

    def from_a(box, c):
        to_a(3 - box, c).wait_recv()
        return ar[box, c]

    def each(low, high, step):
        def one(c, carry):
            step(c)
            return carry

        lax.fori_loop(low, high, one, 0)

    def x_own(k, c):
        snd[2 * k + OTHER, c] = own(2 * k + OTHER, c)
        to_x(k, c).start()

    def share_stats(i):
        return pltpu.make_async_remote_copy(
            src_ref=st0.at[dp], dst_ref=st0.at[dp], send_sem=st0_send.at[i], recv_sem=st0_recv.at[dp],
            device_id={"dp": lax.rem(dp + i, 8)}, device_id_type=MESH_ID,
        )

    def stats_arrival(i):
        peer = lax.rem(dp + i, 8)
        return pltpu.make_async_remote_copy(
            src_ref=st0.at[dp], dst_ref=st0.at[peer], send_sem=st0_send.at[i], recv_sem=st0_recv.at[peer],
            device_id={"dp": peer}, device_id_type=MESH_ID,
        )

    @pl.when(place == 0)
    def _():
        loaded(7, 3)

        def first(c):
            x_own(3, c)

            @pl.when(c < early)
            def _():
                snd[3, c] = own(3, c)
                to_z(3, 0, c).start()

        each(0, pieces, first)
        loaded(1, 6, 5)
        for i in range(1, 8):
            share_stats(i).start()

        def second(c):
            snd[6, c] = own(6, c) + from_x(3, c)
            to_z(6, 3, c).start()
            x_own(2, c)

        each(0, pieces, second)
        loaded(4, 2, 0)

        def send_own_level(c):
            snd[1, c] = own(1, c) + from_z(1, c)
            to_x(0, c).start()

        def third(c):
            snd[4, c] = own(4, c) + from_x(2, c)
            to_z(4, 2, c).start()

        def third_a(c):
            third(c)
            x_own(1, c + early)

        def third_b(c):
            third(c)
            send_own_level(c - early)

        each(0, early, third_a)
        each(early, pieces, third_b)

        def fourth(c):
            snd[2, c] = own(2, c) + from_x(1, c)
            to_z(2, 1, c).start()
            send_own_level(c)

        each(early, pieces, fourth)

        def fifth(c):
            snd[2, c] = own(2, c)
            to_z(2, 1, c).start()

        each(0, early, fifth)

    @pl.when(place == 1)
    def _():
        loaded(7, 1)

        def first(c):
            x_own(3, c)
            snd[1, c] = own(1, c)
            to_z(1, 1, c).start()

        each(0, pieces, first)
        loaded(3, 6, 5)
        for i in range(1, 8):
            share_stats(i).start()
        loaded(4, 2, 0)

        def pass_out(c):
            snd[0, c] = own(0, c) + from_a(0, c)
            to_z(0, 0, c).start()

        def second(c):
            x_own(2, c)
            snd[6, c] = own(6, c) + from_x(3, c) + from_z(3, c)
            to_a(3, c).start()

        def second_b(c):
            second(c)
            pass_out(c - LAG)

        each(0, LAG, second)
        each(LAG, pieces, second_b)

        def third(c):
            snd[4, c] = own(4, c) + from_x(2, c) + from_z(2, c)
            to_a(2, c).start()

        def third_a(c):
            x_own(1, c + early)
            third(c)

            @pl.when(c < LAG)
            def _():
                pass_out(c + pieces - LAG)

        def third_b(c):
            snd[3, c - early] = own(3, c - early) + from_z(0, c - early)
            to_x(1, c - early).start()
            third(c)

        each(0, early, third_a)
        each(early, pieces, third_b)

    total = st0[dp]
    for i in range(1, 8):
        stats_arrival(i).wait_recv()
    total = st0[0]
    for i in range(1, 8):
        total = total + st0[i]
    stats_out[...] = total
    weight_sum = weights[0].astype(jnp.float32)
    for layer in range(1, layers):
        weight_sum = weight_sum + weights[layer].astype(jnp.float32)
    square[...] = jnp.zeros_like(square)
    factors = [weights[layer].astype(jnp.float32) / (weight_sum * total[layer : layer + 1, :]) for layer in range(layers)]

    def finish(layer, c, summed):
        factor = factors[layer]
        gradient = summed * factor
        r = lax.rem(c, per_layer)
        out[layer, pl.ds(pl.multiple_of(r * depth, depth), depth), :] = gradient
        squares = gradient * gradient
        square[...] += jnp.sum(squares.reshape(depth // 8, 8, squares.shape[1]), axis=0)

    @pl.when(place == 0)
    def _():
        for layer in range(layers):
            def last(c, layer=layer):
                finish(layer, c, own(0, c) + from_z(0, c) + from_x(0, c))

            each(layer * per_layer, (layer + 1) * per_layer, last)

    @pl.when(place == 1)
    def _():
        for layer in list(range(layers))[::-1]:
            def last(c, layer=layer):
                finish(layer, c, own(2, c) + from_x(1, c) + from_a(1, c) + from_z(1, c))

            each(layer * per_layer, (layer + 1) * per_layer, last)

    place_in_level = x * n_mp + mp
    level = 2 * n_mp

    def share_square(i):
        peer = lax.rem(place_in_level + i, level)
        return pltpu.make_async_remote_copy(
            src_ref=st1.at[place_in_level], dst_ref=st1.at[place_in_level],
            send_sem=st1_send.at[i], recv_sem=st1_recv.at[place_in_level],
            device_id={"dp": z * 2 + peer // n_mp, "mp": lax.rem(peer, n_mp)}, device_id_type=MESH_ID,
        )

    def square_arrival(i):
        peer = lax.rem(place_in_level + i, level)
        return pltpu.make_async_remote_copy(
            src_ref=st1.at[place_in_level], dst_ref=st1.at[peer], send_sem=st1_send.at[i], recv_sem=st1_recv.at[peer],
            device_id={"dp": z * 2 + peer // n_mp, "mp": lax.rem(peer, n_mp)}, device_id_type=MESH_ID,
        )

    def share_level(i):
        return pltpu.make_async_remote_copy(
            src_ref=st2.at[z], dst_ref=st2.at[z], send_sem=st2_send.at[i], recv_sem=st2_recv.at[z],
            device_id={"dp": lax.rem(z + i, 4) * 2 + x}, device_id_type=MESH_ID,
        )

    def level_arrival(i):
        peer = lax.rem(z + i, 4)
        return pltpu.make_async_remote_copy(
            src_ref=st2.at[z], dst_ref=st2.at[peer], send_sem=st2_send.at[i], recv_sem=st2_recv.at[peer],
            device_id={"dp": peer * 2 + x}, device_id_type=MESH_ID,
        )

    st1[place_in_level] = square[...]
    for i in range(1, level):
        share_square(i).start()
    for i in range(1, level):
        square_arrival(i).wait_recv()
    level_sum = st1[0]
    for i in range(1, level):
        level_sum = level_sum + st1[i]
    st2[z] = level_sum
    for i in range(1, 4):
        share_level(i).start()
    for i in range(1, 4):
        level_arrival(i).wait_recv()
    square_out[...] = jnp.full(square_out.shape, jnp.sum(st2[0] + st2[1] + st2[2] + st2[3]))

    for i in range(1, 8):
        share_stats(i).wait_send()
    for i in range(1, level):
        share_square(i).wait_send()
    for i in range(1, 4):
        share_level(i).wait_send()

    def sent(slot):
        each(0, pieces, lambda c: to_z(slot, 0, c).wait_send())

    for slot in range(1, 8):
        if slot != 2:
            sent(slot)

    @pl.when(place == 0)
    def _():
        sent(2)

    @pl.when(place == 1)
    def _():
        sent(0)


def line_body(n_mp, entries, gradients, layer_mask, exit_losses, exit_weights, params, moment, second):
    layers, rows, columns = params.shape
    depth = min(ROWS, rows)
    pieces = layers * (rows // depth)
    smem = pl.BlockSpec(memory_space=pltpu.SMEM)
    vmem = pl.BlockSpec(memory_space=pltpu.VMEM)
    block = (pieces, depth, columns)
    f32, dma = jnp.float32, pltpu.SemaphoreType.DMA
    tile = (8, columns)

    def kernel(*refs):
        line_kernel(n_mp, *refs)

    gradient, stats, square_sum = pl.pallas_call(
        kernel,
        name="line_reduce",
        out_shape=(
            jax.ShapeDtypeStruct((layers, rows, columns), f32),
            jax.ShapeDtypeStruct(tile, f32),
            jax.ShapeDtypeStruct(tile, f32),
        ),
        in_specs=[smem, smem, smem, pl.BlockSpec(memory_space=pltpu.HBM)],
        out_specs=(vmem, vmem, vmem),
        scratch_shapes=[
            pltpu.VMEM((8, layers, rows, columns), gradients.dtype),
            pltpu.VMEM((8, *block), f32),
            pltpu.VMEM((4, *block), f32),
            pltpu.VMEM((4, *block), f32),
            pltpu.VMEM((2, *block), f32),
            pltpu.VMEM((8, *tile), f32),
            pltpu.VMEM((2 * n_mp, *tile), f32),
            pltpu.VMEM((4, *tile), f32),
            pltpu.VMEM(tile, f32),
            dma((8, layers)), dma((8, pieces)), dma((4, pieces)), dma((4, pieces)), dma((2, pieces)),
            dma((8,)), dma((8,)), dma((2 * n_mp,)), dma((2 * n_mp,)), dma((4,)), dma((4,)),
        ],
        compiler_params=pltpu.CompilerParams(
            collective_id=0, has_side_effects=True, vmem_limit_bytes=32 * 1024 * 1024
        ),
    )(layer_mask, exit_losses, exit_weights, gradients)
    exit_mean = stats[layers : 2 * layers, 0] / stats[:layers, 0]
    new = update(gradient, square_sum[0, 0], entries, params, moment, second)
    return (*new, exit_mean)


def solution(mesh):
    state = P(None, "dp", "mp")
    placed = (P("dp", None, None, "mp"), P("dp", None), P("dp", None), P(), state, state, state)
    n_dp, n_mp = mesh.shape["dp"], mesh.shape["mp"]

    def whole(*args):
        entries = args[4].size
        layers = args[4].shape[0]

        def body(*blocks):
            if n_dp == 8 and layers == 2:
                return line_body(n_mp, entries, *blocks)
            return any_mesh_body(entries, *blocks)

        return jax.shard_map(
            body, mesh=mesh, in_specs=placed, out_specs=(state, state, state, P()), check_vma=False
        )(*args)

    return whole
```

```python
import jax
import jax.numpy as jnp
from jax import lax
from jax.experimental import pallas as pl
from jax.experimental.pallas import tpu as pltpu
from jax.sharding import PartitionSpec as P

max_rms = 1.0
eps_norm = 1e-06
eps_adam = 1e-08
beta_one = 0.9
beta_two = 0.95
learn_rate = 0.01
decay_rate = 0.1

MESH_ID = pl.DeviceIdType.MESH
ROWS = 128
LAG = 2
MINE, OTHER = 0, 1


def update(gradient, clip_scale, params, moment, second):
    clipped = clip_scale * gradient
    new_moment = beta_one * moment + (1.0 - beta_one) * clipped
    new_second = beta_two * second + (1.0 - beta_two) * clipped * clipped
    new_params = params - learn_rate * (
        new_moment / (jnp.sqrt(new_second) + eps_adam) + decay_rate * params
    )
    return new_params, new_moment, new_second


def any_mesh_body(entries, gradients, layer_mask, exit_losses, exit_weights, params, moment, second):
    keep_float = layer_mask[0].astype(jnp.float32)
    loss_terms = keep_float * exit_losses[0]
    local_term = gradients[0].astype(jnp.float32) * keep_float[:, None, None]
    summed = lax.psum_scatter(local_term, "dp", scatter_dimension=1, tiled=True)
    weight_float = exit_weights.astype(jnp.float32)
    weight_sum = jnp.sum(weight_float)
    layer_count, loss_sum = lax.psum((keep_float, loss_terms), "dp")
    gradient = summed * (weight_float / (weight_sum * layer_count))[:, None, None]
    square_sum = lax.psum(jnp.sum(gradient * gradient), ("dp", "mp"))
    rms_value = jnp.sqrt(square_sum / entries)
    clip_scale = jnp.minimum(1.0, max_rms / (rms_value + eps_norm))
    new = update(gradient, clip_scale, params, moment, second)
    return (*new, loss_sum / layer_count)


def line_kernel(
    n_mp, entries, mask_in, losses_in, weights_in, grads, out, stats_out, clip_out,
    mask, losses, weights, held, snd, xr, zr, ar, st0, st1, st2, square,
    small_sem, load_sem, send_sem, x_sem, z_sem, a_sem,
    st0_send, st0_recv, st1_send, st1_recv, st2_send, st2_recv,
):
    layers, rows = out.shape[0], out.shape[1]
    pieces = snd.shape[1]
    depth = snd.shape[2]
    per_layer = pieces // layers
    early = pieces // 2
    dp, mp = lax.axis_index("dp"), lax.axis_index("mp")
    z, x = dp // 2, lax.rem(dp, 2)
    upper = z // 2
    place = lax.rem(z + upper, 2)
    x_dev = z * 2 + 1 - x
    z_dev = (z + 1 - 2 * lax.rem(z, 2)) * 2 + x
    a_dev = (3 - z) * 2 + x

    small = [
        pltpu.make_async_copy(src, dst, small_sem.at[i])
        for i, (src, dst) in enumerate(((mask_in, mask), (losses_in, losses), (weights_in, weights)))
    ]
    for copy in small:
        copy.start()

    def load(slot, layer):
        k, side = slot // 2, slot % 2
        target = (k + upper * (3 - 2 * k)) * 2 + (x if side == MINE else 1 - x)
        return pltpu.make_async_copy(
            grads.at[0, layer, pl.ds(target * rows, rows), :], held.at[slot, layer], load_sem.at[slot, layer]
        )

    order = (7, 3, 1, 6, 5, 4, 2, 0)
    for slot in order:
        for layer in range(layers):
            load(slot, layer).start()

    def loaded(*slots):
        for slot in slots:
            for layer in range(layers):
                load(slot, layer).wait()

    for copy in small:
        copy.wait()
    row = lax.broadcasted_iota(jnp.int32, st0.shape[1:], 0)
    tile = jnp.zeros(st0.shape[1:], jnp.float32)
    for layer in range(layers):
        keep = mask[0, layer].astype(jnp.float32)
        tile = jnp.where(row == layer, keep, tile)
        tile = jnp.where(row == layers + layer, keep * losses[0, layer], tile)
    st0[dp] = tile

    barrier = pltpu.get_barrier_semaphore()
    for i in range(1, 8):
        pl.semaphore_signal(barrier, inc=1, device_id={"dp": lax.rem(dp + i, 8)}, device_id_type=MESH_ID)
    for i in range(1, n_mp):
        for xx in (x, 1 - x):
            pl.semaphore_signal(
                barrier, inc=1, device_id={"dp": z * 2 + xx, "mp": lax.rem(mp + i, n_mp)}, device_id_type=MESH_ID
            )
    pl.semaphore_wait(barrier, 7 + 2 * (n_mp - 1))

    def own(slot, c):
        layer, r = c // per_layer, lax.rem(c, per_layer)
        keep = mask[0, layer].astype(jnp.float32)
        return held[slot, layer, pl.ds(pl.multiple_of(r * depth, depth), depth), :].astype(jnp.float32) * keep

    def push(slot, c, dst, sem, device):
        return pltpu.make_async_remote_copy(
            src_ref=snd.at[slot, c], dst_ref=dst, send_sem=send_sem.at[slot, c], recv_sem=sem,
            device_id={"dp": device}, device_id_type=MESH_ID,
        )

    def to_x(k, c):
        return push(2 * k + OTHER, c, xr.at[k, c], x_sem.at[k, c], x_dev)

    def to_z(slot, box, c):
        return push(slot, c, zr.at[box, c], z_sem.at[box, c], z_dev)

    def to_a(k, c):
        return push(2 * k + MINE, c, ar.at[3 - k, c], a_sem.at[3 - k, c], a_dev)

    def from_x(k, c):
        to_x(k, c).wait_recv()
        return xr[k, c]

    def from_z(box, c):
        to_z(0, box, c).wait_recv()
        return zr[box, c]

    def from_a(box, c):
        to_a(3 - box, c).wait_recv()
        return ar[box, c]

    def each(low, high, step):
        def one(c, carry):
            step(c)
            return carry

        lax.fori_loop(low, high, one, 0)

    def x_own(k, c):
        snd[2 * k + OTHER, c] = own(2 * k + OTHER, c)
        to_x(k, c).start()

    def share_stats(i):
        return pltpu.make_async_remote_copy(
            src_ref=st0.at[dp], dst_ref=st0.at[dp], send_sem=st0_send.at[i], recv_sem=st0_recv.at[dp],
            device_id={"dp": lax.rem(dp + i, 8)}, device_id_type=MESH_ID,
        )

    def stats_arrival(i):
        peer = lax.rem(dp + i, 8)
        return pltpu.make_async_remote_copy(
            src_ref=st0.at[dp], dst_ref=st0.at[peer], send_sem=st0_send.at[i], recv_sem=st0_recv.at[peer],
            device_id={"dp": peer}, device_id_type=MESH_ID,
        )

    @pl.when(place == 0)
    def _():
        loaded(7, 3)

        def first(c):
            x_own(3, c)

            @pl.when(c < early)
            def _():
                snd[3, c] = own(3, c)
                to_z(3, 0, c).start()

        each(0, pieces, first)
        loaded(1, 6, 5)
        for i in range(1, 8):
            share_stats(i).start()

        def second(c):
            snd[6, c] = own(6, c) + from_x(3, c)
            to_z(6, 3, c).start()
            x_own(2, c)

        each(0, pieces, second)
        loaded(4, 2, 0)

        def send_own_level(c):
            snd[1, c] = own(1, c) + from_z(1, c)
            to_x(0, c).start()

        def third(c):
            snd[4, c] = own(4, c) + from_x(2, c)
            to_z(4, 2, c).start()

        def third_a(c):
            third(c)
            x_own(1, c + early)

        def third_b(c):
            third(c)
            send_own_level(c - early)

        each(0, early, third_a)
        each(early, pieces, third_b)

        def fourth(c):
            snd[2, c] = own(2, c) + from_x(1, c)
            to_z(2, 1, c).start()
            send_own_level(c)

        each(early, pieces, fourth)

        def fifth(c):
            snd[2, c] = own(2, c)
            to_z(2, 1, c).start()

        each(0, early, fifth)

    @pl.when(place == 1)
    def _():
        loaded(7, 1)

        def first(c):
            x_own(3, c)
            snd[1, c] = own(1, c)
            to_z(1, 1, c).start()

        each(0, pieces, first)
        loaded(3, 6, 5)
        for i in range(1, 8):
            share_stats(i).start()
        loaded(4, 2, 0)

        def pass_out(c):
            snd[0, c] = own(0, c) + from_a(0, c)
            to_z(0, 0, c).start()

        def second(c):
            x_own(2, c)
            snd[6, c] = own(6, c) + from_x(3, c) + from_z(3, c)
            to_a(3, c).start()

        def second_b(c):
            second(c)
            pass_out(c - LAG)

        each(0, LAG, second)
        each(LAG, pieces, second_b)

        def third(c):
            snd[4, c] = own(4, c) + from_x(2, c) + from_z(2, c)
            to_a(2, c).start()

        def third_a(c):
            x_own(1, c + early)
            third(c)

            @pl.when(c < LAG)
            def _():
                pass_out(c + pieces - LAG)

        def third_b(c):
            snd[3, c - early] = own(3, c - early) + from_z(0, c - early)
            to_x(1, c - early).start()
            third(c)

        each(0, early, third_a)
        each(early, pieces, third_b)

    total = st0[dp]
    for i in range(1, 8):
        stats_arrival(i).wait_recv()
    total = st0[0]
    for i in range(1, 8):
        total = total + st0[i]
    stats_out[...] = total
    weight_sum = weights[0].astype(jnp.float32)
    for layer in range(1, layers):
        weight_sum = weight_sum + weights[layer].astype(jnp.float32)
    square[...] = jnp.zeros_like(square)
    factors = [weights[layer].astype(jnp.float32) / (weight_sum * total[layer : layer + 1, :]) for layer in range(layers)]

    def finish(layer, c, summed):
        factor = factors[layer]
        gradient = summed * factor
        r = lax.rem(c, per_layer)
        out[layer, pl.ds(pl.multiple_of(r * depth, depth), depth), :] = gradient
        squares = gradient * gradient
        square[...] += jnp.sum(squares.reshape(depth // 8, 8, squares.shape[1]), axis=0)

    @pl.when(place == 0)
    def _():
        for layer in range(layers):
            def last(c, layer=layer):
                finish(layer, c, own(0, c) + from_z(0, c) + from_x(0, c))

            each(layer * per_layer, (layer + 1) * per_layer, last)

    @pl.when(place == 1)
    def _():
        for layer in list(range(layers))[::-1]:
            def last(c, layer=layer):
                finish(layer, c, own(2, c) + from_x(1, c) + from_a(1, c) + from_z(1, c))

            each(layer * per_layer, (layer + 1) * per_layer, last)

    place_in_level = x * n_mp + mp
    level = 2 * n_mp

    def share_square(i):
        peer = lax.rem(place_in_level + i, level)
        return pltpu.make_async_remote_copy(
            src_ref=st1.at[place_in_level], dst_ref=st1.at[place_in_level],
            send_sem=st1_send.at[i], recv_sem=st1_recv.at[place_in_level],
            device_id={"dp": z * 2 + peer // n_mp, "mp": lax.rem(peer, n_mp)}, device_id_type=MESH_ID,
        )

    def square_arrival(i):
        peer = lax.rem(place_in_level + i, level)
        return pltpu.make_async_remote_copy(
            src_ref=st1.at[place_in_level], dst_ref=st1.at[peer], send_sem=st1_send.at[i], recv_sem=st1_recv.at[peer],
            device_id={"dp": z * 2 + peer // n_mp, "mp": lax.rem(peer, n_mp)}, device_id_type=MESH_ID,
        )

    def share_level(i):
        return pltpu.make_async_remote_copy(
            src_ref=st2.at[z], dst_ref=st2.at[z], send_sem=st2_send.at[i], recv_sem=st2_recv.at[z],
            device_id={"dp": lax.rem(z + i, 4) * 2 + x}, device_id_type=MESH_ID,
        )

    def level_arrival(i):
        peer = lax.rem(z + i, 4)
        return pltpu.make_async_remote_copy(
            src_ref=st2.at[z], dst_ref=st2.at[peer], send_sem=st2_send.at[i], recv_sem=st2_recv.at[peer],
            device_id={"dp": peer * 2 + x}, device_id_type=MESH_ID,
        )

    st1[place_in_level] = square[...]
    for i in range(1, level):
        share_square(i).start()
    for i in range(1, level):
        square_arrival(i).wait_recv()
    level_sum = st1[0]
    for i in range(1, level):
        level_sum = level_sum + st1[i]
    st2[z] = level_sum
    for i in range(1, 4):
        share_level(i).start()
    for i in range(1, 4):
        level_arrival(i).wait_recv()
    square_sum = jnp.sum(st2[0] + st2[1] + st2[2] + st2[3], keepdims=True)
    rms_value = jnp.sqrt(square_sum / entries)
    clip_out[...] = jnp.broadcast_to(jnp.minimum(1.0, max_rms / (rms_value + eps_norm)), clip_out.shape)

    for i in range(1, 8):
        share_stats(i).wait_send()
    for i in range(1, level):
        share_square(i).wait_send()
    for i in range(1, 4):
        share_level(i).wait_send()

    def sent(slot):
        each(0, pieces, lambda c: to_z(slot, 0, c).wait_send())

    for slot in range(1, 8):
        if slot != 2:
            sent(slot)

    @pl.when(place == 0)
    def _():
        sent(2)

    @pl.when(place == 1)
    def _():
        sent(0)


def line_body(n_mp, entries, gradients, layer_mask, exit_losses, exit_weights, params, moment, second):
    layers, rows, columns = params.shape
    depth = min(ROWS, rows)
    pieces = layers * (rows // depth)
    vmem = pl.BlockSpec(memory_space=pltpu.VMEM)
    block = (pieces, depth, columns)
    f32, dma = jnp.float32, pltpu.SemaphoreType.DMA
    tile = (8, columns)

    def kernel(*refs):
        line_kernel(n_mp, entries, *refs)

    gradient, stats, clip = pl.pallas_call(
        kernel,
        name="line_reduce",
        out_shape=(
            jax.ShapeDtypeStruct((layers, rows, columns), f32),
            jax.ShapeDtypeStruct(tile, f32),
            jax.ShapeDtypeStruct((1, columns), f32),
        ),
        in_specs=[pl.BlockSpec(memory_space=pltpu.HBM)] * 4,
        out_specs=(vmem, vmem, vmem),
        scratch_shapes=[
            pltpu.SMEM(layer_mask.shape, layer_mask.dtype),
            pltpu.SMEM(exit_losses.shape, exit_losses.dtype),
            pltpu.SMEM(exit_weights.shape, exit_weights.dtype),
            pltpu.VMEM((8, layers, rows, columns), gradients.dtype),
            pltpu.VMEM((8, *block), f32),
            pltpu.VMEM((4, *block), f32),
            pltpu.VMEM((4, *block), f32),
            pltpu.VMEM((2, *block), f32),
            pltpu.VMEM((8, *tile), f32),
            pltpu.VMEM((2 * n_mp, *tile), f32),
            pltpu.VMEM((4, *tile), f32),
            pltpu.VMEM(tile, f32),
            dma((3,)), dma((8, layers)), dma((8, pieces)), dma((4, pieces)), dma((4, pieces)), dma((2, pieces)),
            dma((8,)), dma((8,)), dma((2 * n_mp,)), dma((2 * n_mp,)), dma((4,)), dma((4,)),
        ],
        compiler_params=pltpu.CompilerParams(
            collective_id=0, has_side_effects=True, vmem_limit_bytes=32 * 1024 * 1024
        ),
    )(*(pltpu.with_memory_space_constraint(a, pltpu.HBM) for a in (layer_mask, exit_losses, exit_weights, gradients)))
    exit_mean = stats[layers : 2 * layers, 0] / stats[:layers, 0]
    new = update(gradient, clip[None], params, moment, second)
    return (*new, exit_mean)


def solution(mesh):
    state = P(None, "dp", "mp")
    placed = (P("dp", None, None, "mp"), P("dp", None), P("dp", None), P(), state, state, state)
    n_dp, n_mp = mesh.shape["dp"], mesh.shape["mp"]

    def whole(*args):
        entries = args[4].size
        layers = args[4].shape[0]

        def body(*blocks):
            if n_dp == 8 and layers == 2:
                return line_body(n_mp, entries, *blocks)
            return any_mesh_body(entries, *blocks)

        return jax.shard_map(
            body, mesh=mesh, in_specs=placed, out_specs=(state, state, state, P()), check_vma=False
        )(*args)

    return whole
```

```python
import jax
import jax.numpy as jnp
from jax import lax
from jax.experimental import pallas as pl
from jax.experimental.pallas import tpu as pltpu
from jax.sharding import PartitionSpec as P

max_rms = 1.0
eps_norm = 1e-06
eps_adam = 1e-08
beta_one = 0.9
beta_two = 0.95
learn_rate = 0.01
decay_rate = 0.1

MESH_ID = pl.DeviceIdType.MESH
ROWS = 256
LANES = 128
LAG = 1
MINE, OTHER = 0, 1


def update(gradient, clip_scale, params, moment, second):
    clipped = clip_scale * gradient
    new_moment = beta_one * moment + (1.0 - beta_one) * clipped
    new_second = beta_two * second + (1.0 - beta_two) * clipped * clipped
    new_params = params - learn_rate * (
        new_moment / (jnp.sqrt(new_second) + eps_adam) + decay_rate * params
    )
    return new_params, new_moment, new_second


def any_mesh_body(entries, gradients, layer_mask, exit_losses, exit_weights, params, moment, second):
    keep_float = layer_mask[0].astype(jnp.float32)
    loss_terms = keep_float * exit_losses[0]
    local_term = gradients[0].astype(jnp.float32) * keep_float[:, None, None]
    summed = lax.psum_scatter(local_term, "dp", scatter_dimension=1, tiled=True)
    weight_float = exit_weights.astype(jnp.float32)
    weight_sum = jnp.sum(weight_float)
    layer_count, loss_sum = lax.psum((keep_float, loss_terms), "dp")
    gradient = summed * (weight_float / (weight_sum * layer_count))[:, None, None]
    square_sum = lax.psum(jnp.sum(gradient * gradient), ("dp", "mp"))
    rms_value = jnp.sqrt(square_sum / entries)
    clip_scale = jnp.minimum(1.0, max_rms / (rms_value + eps_norm))
    new = update(gradient, clip_scale, params, moment, second)
    return (*new, loss_sum / layer_count)


def line_kernel(
    n_mp, entries, mask_in, losses_in, weights_in, grads, out, stats_out, clip_out,
    mask, losses, weights, held, snd, xr, zr, ar, st0, st1, st2, square,
    small_sem, load_sem, send_sem, x_sem, z_sem, a_sem,
    st0_send, st0_recv, st1_send, st1_recv, st2_send, st2_recv,
):
    layers, rows = out.shape[0], out.shape[1]
    pieces = snd.shape[1]
    depth = snd.shape[2]
    per_layer = pieces // layers
    early = pieces // 2
    dp, mp = lax.axis_index("dp"), lax.axis_index("mp")
    z, x = dp // 2, lax.rem(dp, 2)
    upper = z // 2
    place = lax.rem(z + upper, 2)
    x_dev = z * 2 + 1 - x
    z_dev = (z + 1 - 2 * lax.rem(z, 2)) * 2 + x
    a_dev = (3 - z) * 2 + x

    barrier = pltpu.get_barrier_semaphore()
    for i in range(1, 8):
        pl.semaphore_signal(barrier, inc=1, device_id={"dp": lax.rem(dp + i, 8)}, device_id_type=MESH_ID)
    for i in range(1, n_mp):
        for xx in (x, 1 - x):
            pl.semaphore_signal(
                barrier, inc=1, device_id={"dp": z * 2 + xx, "mp": lax.rem(mp + i, n_mp)}, device_id_type=MESH_ID
            )

    small = [
        pltpu.make_async_copy(src, dst, small_sem.at[i])
        for i, (src, dst) in enumerate(((mask_in, mask), (losses_in, losses), (weights_in, weights)))
    ]
    for copy in small:
        copy.start()

    def load(slot, layer):
        k, side = slot // 2, slot % 2
        target = (k + upper * (3 - 2 * k)) * 2 + (x if side == MINE else 1 - x)
        return pltpu.make_async_copy(
            grads.at[0, layer, pl.ds(target * rows, rows), :], held.at[slot, layer], load_sem.at[slot, layer]
        )

    order = (7, 3, 1, 6, 5, 4, 2, 0)
    for slot in order:
        for layer in range(layers):
            load(slot, layer).start()

    def loaded(*slots):
        for slot in slots:
            for layer in range(layers):
                load(slot, layer).wait()

    for copy in small:
        copy.wait()
    row = lax.broadcasted_iota(jnp.int32, st0.shape[1:], 0)
    tile = jnp.zeros(st0.shape[1:], jnp.float32)
    for layer in range(layers):
        keep = mask[0, layer].astype(jnp.float32)
        tile = jnp.where(row == layer, keep, tile)
        tile = jnp.where(row == layers + layer, keep * losses[0, layer], tile)
    st0[dp] = tile

    pl.semaphore_wait(barrier, 7 + 2 * (n_mp - 1))

    def own(slot, c):
        layer, r = c // per_layer, lax.rem(c, per_layer)
        keep = mask[0, layer].astype(jnp.float32)
        return held[slot, layer, pl.ds(pl.multiple_of(r * depth, depth), depth), :].astype(jnp.float32) * keep

    def push(slot, c, dst, sem, device):
        return pltpu.make_async_remote_copy(
            src_ref=snd.at[slot, c], dst_ref=dst, send_sem=send_sem.at[slot, c], recv_sem=sem,
            device_id={"dp": device}, device_id_type=MESH_ID,
        )

    def to_x(k, c):
        return push(2 * k + OTHER, c, xr.at[k, c], x_sem.at[k, c], x_dev)

    def to_z(slot, box, c):
        return push(slot, c, zr.at[box, c], z_sem.at[box, c], z_dev)

    def to_a(k, c):
        return push(2 * k + MINE, c, ar.at[3 - k, c], a_sem.at[3 - k, c], a_dev)

    def from_x(k, c):
        to_x(k, c).wait_recv()
        return xr[k, c]

    def from_z(box, c):
        to_z(0, box, c).wait_recv()
        return zr[box, c]

    def from_a(box, c):
        to_a(3 - box, c).wait_recv()
        return ar[box, c]

    def each(low, high, step):
        def one(c, carry):
            step(c)
            return carry

        lax.fori_loop(low, high, one, 0)

    def x_own(k, c):
        snd[2 * k + OTHER, c] = own(2 * k + OTHER, c)
        to_x(k, c).start()

    def share_stats(i):
        return pltpu.make_async_remote_copy(
            src_ref=st0.at[dp], dst_ref=st0.at[dp], send_sem=st0_send.at[i], recv_sem=st0_recv.at[dp],
            device_id={"dp": lax.rem(dp + i, 8)}, device_id_type=MESH_ID,
        )

    def stats_arrival(i):
        peer = lax.rem(dp + i, 8)
        return pltpu.make_async_remote_copy(
            src_ref=st0.at[dp], dst_ref=st0.at[peer], send_sem=st0_send.at[i], recv_sem=st0_recv.at[peer],
            device_id={"dp": peer}, device_id_type=MESH_ID,
        )

    @pl.when(place == 0)
    def _():
        loaded(7, 3)

        def first(c):
            x_own(3, c)

            @pl.when(c < early)
            def _():
                snd[3, c] = own(3, c)
                to_z(3, 0, c).start()

        each(0, pieces, first)
        loaded(1, 6, 5)
        for i in range(1, 8):
            share_stats(i).start()

        def second(c):
            snd[6, c] = own(6, c) + from_x(3, c)
            to_z(6, 3, c).start()
            x_own(2, c)

        each(0, pieces, second)
        loaded(4, 2, 0)

        def send_own_level(c):
            snd[1, c] = own(1, c) + from_z(1, c)
            to_x(0, c).start()

        def third(c):
            snd[4, c] = own(4, c) + from_x(2, c)
            to_z(4, 2, c).start()

        def third_a(c):
            third(c)
            x_own(1, c + early)

        def third_b(c):
            third(c)
            send_own_level(c - (pieces - early))

        each(0, pieces - early, third_a)
        each(pieces - early, pieces, third_b)

        def fourth(c):
            snd[2, c] = own(2, c) + from_x(1, c)
            to_z(2, 1, c).start()
            send_own_level(c)

        each(early, pieces, fourth)

        def fifth(c):
            snd[2, c] = own(2, c)
            to_z(2, 1, c).start()

        each(0, early, fifth)

    @pl.when(place == 1)
    def _():
        loaded(7, 1)

        def first(c):
            x_own(3, c)
            snd[1, c] = own(1, c)
            to_z(1, 1, c).start()

        each(0, pieces, first)
        loaded(3, 6, 5)
        for i in range(1, 8):
            share_stats(i).start()
        loaded(4, 2, 0)

        def pass_out(c):
            snd[0, c] = own(0, c) + from_a(0, c)
            to_z(0, 0, c).start()

        def second(c):
            x_own(2, c)
            snd[6, c] = own(6, c) + from_x(3, c) + from_z(3, c)
            to_a(3, c).start()

        def second_b(c):
            second(c)
            pass_out(c - LAG)

        each(0, LAG, second)
        each(LAG, pieces, second_b)

        def third(c):
            snd[4, c] = own(4, c) + from_x(2, c) + from_z(2, c)
            to_a(2, c).start()

        def third_a(c):
            x_own(1, c + early)
            third(c)

            @pl.when(c < LAG)
            def _():
                pass_out(c + pieces - LAG)

        def third_b(c):
            late = c - (pieces - early)
            snd[3, late] = own(3, late) + from_z(0, late)
            to_x(1, late).start()
            third(c)

        each(0, pieces - early, third_a)
        each(pieces - early, pieces, third_b)

    total = st0[dp]
    for i in range(1, 8):
        stats_arrival(i).wait_recv()
    total = st0[0]
    for i in range(1, 8):
        total = total + st0[i]
    stats_out[...] = total
    weight_sum = weights[0].astype(jnp.float32)
    for layer in range(1, layers):
        weight_sum = weight_sum + weights[layer].astype(jnp.float32)
    square[...] = jnp.zeros_like(square)
    factors = [weights[layer].astype(jnp.float32) / (weight_sum * total[layer : layer + 1, :]) for layer in range(layers)]

    def finish(layer, c, summed):
        factor = factors[layer]
        gradient = summed * factor
        r = lax.rem(c, per_layer)
        out[layer, pl.ds(pl.multiple_of(r * depth, depth), depth), :] = gradient
        squares = gradient * gradient
        square[...] += jnp.sum(squares.reshape(depth // 8, 8, squares.shape[1]), axis=0)

    @pl.when(place == 0)
    def _():
        for layer in range(layers):
            def last(c, layer=layer):
                finish(layer, c, own(0, c) + from_z(0, c) + from_x(0, c))

            each(layer * per_layer, (layer + 1) * per_layer, last)

    @pl.when(place == 1)
    def _():
        for layer in list(range(layers))[::-1]:
            def last(c, layer=layer):
                finish(layer, c, own(2, c) + from_x(1, c) + from_a(1, c) + from_z(1, c))

            each(layer * per_layer, (layer + 1) * per_layer, last)

    place_in_level = x * n_mp + mp
    level = 2 * n_mp

    def share_square(i):
        peer = lax.rem(place_in_level + i, level)
        return pltpu.make_async_remote_copy(
            src_ref=st1.at[place_in_level], dst_ref=st1.at[place_in_level],
            send_sem=st1_send.at[i], recv_sem=st1_recv.at[place_in_level],
            device_id={"dp": z * 2 + peer // n_mp, "mp": lax.rem(peer, n_mp)}, device_id_type=MESH_ID,
        )

    def square_arrival(i):
        peer = lax.rem(place_in_level + i, level)
        return pltpu.make_async_remote_copy(
            src_ref=st1.at[place_in_level], dst_ref=st1.at[peer], send_sem=st1_send.at[i], recv_sem=st1_recv.at[peer],
            device_id={"dp": z * 2 + peer // n_mp, "mp": lax.rem(peer, n_mp)}, device_id_type=MESH_ID,
        )

    def share_level(i):
        return pltpu.make_async_remote_copy(
            src_ref=st2.at[z], dst_ref=st2.at[z], send_sem=st2_send.at[i], recv_sem=st2_recv.at[z],
            device_id={"dp": lax.rem(z + i, 4) * 2 + x}, device_id_type=MESH_ID,
        )

    def level_arrival(i):
        peer = lax.rem(z + i, 4)
        return pltpu.make_async_remote_copy(
            src_ref=st2.at[z], dst_ref=st2.at[peer], send_sem=st2_send.at[i], recv_sem=st2_recv.at[peer],
            device_id={"dp": peer * 2 + x}, device_id_type=MESH_ID,
        )

    folded = jnp.sum(square[...], axis=0, keepdims=True)
    st1[place_in_level] = sum(folded[:, i : i + LANES] for i in range(0, folded.shape[1], LANES))
    for i in range(1, level):
        share_square(i).start()
    for i in range(1, level):
        square_arrival(i).wait_recv()
    level_sum = st1[0]
    for i in range(1, level):
        level_sum = level_sum + st1[i]
    st2[z] = level_sum
    for i in range(1, 4):
        share_level(i).start()
    for i in range(1, 4):
        level_arrival(i).wait_recv()
    square_sum = jnp.sum(st2[0] + st2[1] + st2[2] + st2[3], keepdims=True)
    rms_value = jnp.sqrt(square_sum / entries)
    clip_out[...] = jnp.broadcast_to(jnp.minimum(1.0, max_rms / (rms_value + eps_norm)), clip_out.shape)

    for i in range(1, 8):
        share_stats(i).wait_send()
    for i in range(1, level):
        share_square(i).wait_send()
    for i in range(1, 4):
        share_level(i).wait_send()

    def sent(slot):
        each(0, pieces, lambda c: to_z(slot, 0, c).wait_send())

    for slot in range(1, 8):
        if slot != 2:
            sent(slot)

    @pl.when(place == 0)
    def _():
        sent(2)

    @pl.when(place == 1)
    def _():
        sent(0)


def line_body(n_mp, entries, gradients, layer_mask, exit_losses, exit_weights, params, moment, second):
    layers, rows, columns = params.shape
    depth = min(ROWS, rows)
    pieces = layers * (rows // depth)
    vmem = pl.BlockSpec(memory_space=pltpu.VMEM)
    block = (pieces, depth, columns)
    f32, dma = jnp.float32, pltpu.SemaphoreType.DMA
    tile = (8, columns)

    def kernel(*refs):
        line_kernel(n_mp, entries, *refs)

    gradient, stats, clip = pl.pallas_call(
        kernel,
        name="line_reduce",
        out_shape=(
            jax.ShapeDtypeStruct((layers, rows, columns), f32),
            jax.ShapeDtypeStruct(tile, f32),
            jax.ShapeDtypeStruct((1, columns), f32),
        ),
        in_specs=[pl.BlockSpec(memory_space=pltpu.HBM)] * 4,
        out_specs=(vmem, vmem, vmem),
        scratch_shapes=[
            pltpu.SMEM(layer_mask.shape, layer_mask.dtype),
            pltpu.SMEM(exit_losses.shape, exit_losses.dtype),
            pltpu.SMEM(exit_weights.shape, exit_weights.dtype),
            pltpu.VMEM((8, layers, rows, columns), gradients.dtype),
            pltpu.VMEM((8, *block), f32),
            pltpu.VMEM((4, *block), f32),
            pltpu.VMEM((4, *block), f32),
            pltpu.VMEM((2, *block), f32),
            pltpu.VMEM((8, *tile), f32),
            pltpu.VMEM((2 * n_mp, 1, LANES), f32),
            pltpu.VMEM((4, 1, LANES), f32),
            pltpu.VMEM(tile, f32),
            dma((3,)), dma((8, layers)), dma((8, pieces)), dma((4, pieces)), dma((4, pieces)), dma((2, pieces)),
            dma((8,)), dma((8,)), dma((2 * n_mp,)), dma((2 * n_mp,)), dma((4,)), dma((4,)),
        ],
        compiler_params=pltpu.CompilerParams(
            collective_id=0, has_side_effects=True, vmem_limit_bytes=32 * 1024 * 1024
        ),
    )(*(pltpu.with_memory_space_constraint(a, pltpu.HBM) for a in (layer_mask, exit_losses, exit_weights, gradients)))
    exit_mean = stats[layers : 2 * layers, 0] / stats[:layers, 0]
    new = update(gradient, clip[None], params, moment, second)
    return (*new, exit_mean)


def solution(mesh):
    state = P(None, "dp", "mp")
    placed = (P("dp", None, None, "mp"), P("dp", None), P("dp", None), P(), state, state, state)
    n_dp, n_mp = mesh.shape["dp"], mesh.shape["mp"]

    def whole(*args):
        entries = args[4].size
        layers = args[4].shape[0]

        def body(*blocks):
            if n_dp == 8 and layers == 2:
                return line_body(n_mp, entries, *blocks)
            return any_mesh_body(entries, *blocks)

        return jax.shard_map(
            body, mesh=mesh, in_specs=placed, out_specs=(state, state, state, P()), check_vma=False
        )(*args)

    return whole
```

```python
import jax
import jax.numpy as jnp
from jax import lax
from jax.experimental import pallas as pl
from jax.experimental.pallas import tpu as pltpu
from jax.sharding import PartitionSpec as P

max_rms = 1.0
eps_norm = 1e-06
eps_adam = 1e-08
beta_one = 0.9
beta_two = 0.95
learn_rate = 0.01
decay_rate = 0.1

MESH_ID = pl.DeviceIdType.MESH
ROWS = 256
LANES = 128
LAG = 1
MINE, OTHER = 0, 1


def update(gradient, clip_scale, params, moment, second):
    clipped = clip_scale * gradient
    new_moment = beta_one * moment + (1.0 - beta_one) * clipped
    new_second = beta_two * second + (1.0 - beta_two) * clipped * clipped
    new_params = params - learn_rate * (
        new_moment / (jnp.sqrt(new_second) + eps_adam) + decay_rate * params
    )
    return new_params, new_moment, new_second


def any_mesh_body(entries, gradients, layer_mask, exit_losses, exit_weights, params, moment, second):
    keep_float = layer_mask[0].astype(jnp.float32)
    loss_terms = keep_float * exit_losses[0]
    local_term = gradients[0].astype(jnp.float32) * keep_float[:, None, None]
    summed = lax.psum_scatter(local_term, "dp", scatter_dimension=1, tiled=True)
    weight_float = exit_weights.astype(jnp.float32)
    weight_sum = jnp.sum(weight_float)
    layer_count, loss_sum = lax.psum((keep_float, loss_terms), "dp")
    gradient = summed * (weight_float / (weight_sum * layer_count))[:, None, None]
    square_sum = lax.psum(jnp.sum(gradient * gradient), ("dp", "mp"))
    rms_value = jnp.sqrt(square_sum / entries)
    clip_scale = jnp.minimum(1.0, max_rms / (rms_value + eps_norm))
    new = update(gradient, clip_scale, params, moment, second)
    return (*new, loss_sum / layer_count)


def line_kernel(
    n_mp, entries, mask_in, losses_in, weights_in, grads, out, stats_out, clip_out,
    mask, losses, weights, held, snd, xr, zr, ar, st0, st1, square,
    small_sem, load_sem, send_sem, x_sem, z_sem, a_sem,
    st0_send, st0_recv, st1_send, st1_recv,
):
    layers, rows = out.shape[0], out.shape[1]
    pieces = snd.shape[1]
    depth = snd.shape[2]
    per_layer = pieces // layers
    early = pieces // 2
    dp, mp = lax.axis_index("dp"), lax.axis_index("mp")
    z, x = dp // 2, lax.rem(dp, 2)
    upper = z // 2
    place = lax.rem(z + upper, 2)
    x_dev = z * 2 + 1 - x
    z_dev = (z + 1 - 2 * lax.rem(z, 2)) * 2 + x
    a_dev = (3 - z) * 2 + x

    barrier = pltpu.get_barrier_semaphore()
    devices = 8 * n_mp
    place_in_all = dp * n_mp + mp

    def away(i):
        peer = lax.rem(place_in_all + i, devices)
        return peer, {"dp": peer // n_mp, "mp": lax.rem(peer, n_mp)}

    for i in range(1, devices):
        pl.semaphore_signal(barrier, inc=1, device_id=away(i)[1], device_id_type=MESH_ID)

    small = [
        pltpu.make_async_copy(src, dst, small_sem.at[i])
        for i, (src, dst) in enumerate(((mask_in, mask), (losses_in, losses), (weights_in, weights)))
    ]
    for copy in small:
        copy.start()

    def load(slot, layer):
        k, side = slot // 2, slot % 2
        target = (k + upper * (3 - 2 * k)) * 2 + (x if side == MINE else 1 - x)
        return pltpu.make_async_copy(
            grads.at[0, layer, pl.ds(target * rows, rows), :], held.at[slot, layer], load_sem.at[slot, layer]
        )

    order = (7, 3, 1, 6, 5, 4, 2, 0)
    for slot in order:
        for layer in range(layers):
            load(slot, layer).start()

    def loaded(*slots):
        for slot in slots:
            for layer in range(layers):
                load(slot, layer).wait()

    for copy in small:
        copy.wait()
    lane = lax.broadcasted_iota(jnp.int32, st0.shape[1:], 1)
    tile = jnp.zeros(st0.shape[1:], jnp.float32)
    for layer in range(layers):
        keep = mask[0, layer].astype(jnp.float32)
        tile = jnp.where(lane == layer, keep, tile)
        tile = jnp.where(lane == layers + layer, keep * losses[0, layer], tile)
    st0[dp] = tile

    pl.semaphore_wait(barrier, devices - 1)

    def own(slot, c):
        layer, r = c // per_layer, lax.rem(c, per_layer)
        keep = mask[0, layer].astype(jnp.float32)
        return held[slot, layer, pl.ds(pl.multiple_of(r * depth, depth), depth), :].astype(jnp.float32) * keep

    def push(slot, c, dst, sem, device):
        return pltpu.make_async_remote_copy(
            src_ref=snd.at[slot, c], dst_ref=dst, send_sem=send_sem.at[slot, c], recv_sem=sem,
            device_id={"dp": device}, device_id_type=MESH_ID,
        )

    def to_x(k, c):
        return push(2 * k + OTHER, c, xr.at[k, c], x_sem.at[k, c], x_dev)

    def to_z(slot, box, c):
        return push(slot, c, zr.at[box, c], z_sem.at[box, c], z_dev)

    def to_a(k, c):
        return push(2 * k + MINE, c, ar.at[3 - k, c], a_sem.at[3 - k, c], a_dev)

    def from_x(k, c):
        to_x(k, c).wait_recv()
        return xr[k, c]

    def from_z(box, c):
        to_z(0, box, c).wait_recv()
        return zr[box, c]

    def from_a(box, c):
        to_a(3 - box, c).wait_recv()
        return ar[box, c]

    def each(low, high, step):
        def one(c, carry):
            step(c)
            return carry

        lax.fori_loop(low, high, one, 0)

    def x_own(k, c):
        snd[2 * k + OTHER, c] = own(2 * k + OTHER, c)
        to_x(k, c).start()

    def share_stats(i):
        return pltpu.make_async_remote_copy(
            src_ref=st0.at[dp], dst_ref=st0.at[dp], send_sem=st0_send.at[i], recv_sem=st0_recv.at[dp],
            device_id={"dp": lax.rem(dp + i, 8)}, device_id_type=MESH_ID,
        )

    def stats_arrival(i):
        peer = lax.rem(dp + i, 8)
        return pltpu.make_async_remote_copy(
            src_ref=st0.at[dp], dst_ref=st0.at[peer], send_sem=st0_send.at[i], recv_sem=st0_recv.at[peer],
            device_id={"dp": peer}, device_id_type=MESH_ID,
        )

    @pl.when(place == 0)
    def _():
        loaded(7, 3)

        def first(c):
            x_own(3, c)

            @pl.when(c < early)
            def _():
                snd[3, c] = own(3, c)
                to_z(3, 0, c).start()

        each(0, pieces, first)
        loaded(1, 6, 5)
        for i in range(1, 8):
            share_stats(i).start()

        def second(c):
            snd[6, c] = own(6, c) + from_x(3, c)
            to_z(6, 3, c).start()
            x_own(2, c)

        each(0, pieces, second)
        loaded(4, 2, 0)

        def send_own_level(c):
            snd[1, c] = own(1, c) + from_z(1, c)
            to_x(0, c).start()

        def third(c):
            snd[4, c] = own(4, c) + from_x(2, c)
            to_z(4, 2, c).start()

        def third_a(c):
            third(c)
            x_own(1, c + early)

        def third_b(c):
            third(c)
            send_own_level(c - (pieces - early))

        each(0, pieces - early, third_a)
        each(pieces - early, pieces, third_b)

        def fourth(c):
            snd[2, c] = own(2, c) + from_x(1, c)
            to_z(2, 1, c).start()
            send_own_level(c)

        each(early, pieces, fourth)

        def fifth(c):
            snd[2, c] = own(2, c)
            to_z(2, 1, c).start()

        each(0, early, fifth)

    @pl.when(place == 1)
    def _():
        loaded(7, 1)

        def first(c):
            x_own(3, c)
            snd[1, c] = own(1, c)
            to_z(1, 1, c).start()

        each(0, pieces, first)
        loaded(3, 6, 5)
        for i in range(1, 8):
            share_stats(i).start()
        loaded(4, 2, 0)

        def pass_out(c):
            snd[0, c] = own(0, c) + from_a(0, c)
            to_z(0, 0, c).start()

        def second(c):
            x_own(2, c)
            snd[6, c] = own(6, c) + from_x(3, c) + from_z(3, c)
            to_a(3, c).start()

        def second_b(c):
            second(c)
            pass_out(c - LAG)

        each(0, LAG, second)
        each(LAG, pieces, second_b)

        def third(c):
            snd[4, c] = own(4, c) + from_x(2, c) + from_z(2, c)
            to_a(2, c).start()

        def third_a(c):
            x_own(1, c + early)
            third(c)

            @pl.when(c < LAG)
            def _():
                pass_out(c + pieces - LAG)

        def third_b(c):
            late = c - (pieces - early)
            snd[3, late] = own(3, late) + from_z(0, late)
            to_x(1, late).start()
            third(c)

        each(0, pieces - early, third_a)
        each(pieces - early, pieces, third_b)

    for i in range(1, 8):
        stats_arrival(i).wait_recv()
    total = st0[0]
    for i in range(1, 8):
        total = total + st0[i]
    stats_out[...] = total
    weight_sum = weights[0].astype(jnp.float32)
    for layer in range(1, layers):
        weight_sum = weight_sum + weights[layer].astype(jnp.float32)
    square[...] = jnp.zeros_like(square)
    factors = [weights[layer].astype(jnp.float32) / (weight_sum * total[:, layer : layer + 1]) for layer in range(layers)]

    def finish(layer, c, summed):
        factor = factors[layer]
        gradient = summed * factor
        r = lax.rem(c, per_layer)
        out[layer, pl.ds(pl.multiple_of(r * depth, depth), depth), :] = gradient
        squares = gradient * gradient
        square[...] += jnp.sum(squares.reshape(depth // 8, 8, squares.shape[1]), axis=0)

    @pl.when(place == 0)
    def _():
        for layer in range(layers):
            def last(c, layer=layer):
                finish(layer, c, own(0, c) + from_z(0, c) + from_x(0, c))

            each(layer * per_layer, (layer + 1) * per_layer, last)

    @pl.when(place == 1)
    def _():
        for layer in list(range(layers))[::-1]:
            def last(c, layer=layer):
                finish(layer, c, own(2, c) + from_x(1, c) + from_a(1, c) + from_z(1, c))

            each(layer * per_layer, (layer + 1) * per_layer, last)

    def share_square(i):
        return pltpu.make_async_remote_copy(
            src_ref=st1.at[place_in_all], dst_ref=st1.at[place_in_all],
            send_sem=st1_send.at[i], recv_sem=st1_recv.at[place_in_all],
            device_id=away(i)[1], device_id_type=MESH_ID,
        )

    def square_arrival(i):
        peer, device = away(i)
        return pltpu.make_async_remote_copy(
            src_ref=st1.at[place_in_all], dst_ref=st1.at[peer], send_sem=st1_send.at[i], recv_sem=st1_recv.at[peer],
            device_id=device, device_id_type=MESH_ID,
        )

    folded = jnp.sum(square[...], axis=0, keepdims=True)
    st1[place_in_all] = sum(folded[:, i : i + LANES] for i in range(0, folded.shape[1], LANES))
    for i in range(1, devices):
        share_square(i).start()
    for i in range(1, devices):
        square_arrival(i).wait_recv()
    all_rows = st1[0]
    for i in range(1, devices):
        all_rows = all_rows + st1[i]
    square_sum = jnp.sum(all_rows, keepdims=True)
    rms_value = jnp.sqrt(square_sum / entries)
    clip_out[...] = jnp.broadcast_to(jnp.minimum(1.0, max_rms / (rms_value + eps_norm)), clip_out.shape)

    for i in range(1, 8):
        share_stats(i).wait_send()
    for i in range(1, devices):
        share_square(i).wait_send()

    def sent(slot):
        each(0, pieces, lambda c: to_z(slot, 0, c).wait_send())

    for slot in range(1, 8):
        if slot != 2:
            sent(slot)

    @pl.when(place == 0)
    def _():
        sent(2)

    @pl.when(place == 1)
    def _():
        sent(0)


def line_body(n_mp, entries, gradients, layer_mask, exit_losses, exit_weights, params, moment, second):
    layers, rows, columns = params.shape
    depth = min(ROWS, rows)
    pieces = layers * (rows // depth)
    vmem = pl.BlockSpec(memory_space=pltpu.VMEM)
    block = (pieces, depth, columns)
    f32, dma = jnp.float32, pltpu.SemaphoreType.DMA
    tile = (8, columns)

    def kernel(*refs):
        line_kernel(n_mp, entries, *refs)

    gradient, stats, clip = pl.pallas_call(
        kernel,
        name="line_reduce",
        out_shape=(
            jax.ShapeDtypeStruct((layers, rows, columns), f32),
            jax.ShapeDtypeStruct((1, LANES), f32),
            jax.ShapeDtypeStruct((1, columns), f32),
        ),
        in_specs=[pl.BlockSpec(memory_space=pltpu.HBM)] * 4,
        out_specs=(vmem, vmem, vmem),
        scratch_shapes=[
            pltpu.SMEM(layer_mask.shape, layer_mask.dtype),
            pltpu.SMEM(exit_losses.shape, exit_losses.dtype),
            pltpu.SMEM(exit_weights.shape, exit_weights.dtype),
            pltpu.VMEM((8, layers, rows, columns), gradients.dtype),
            pltpu.VMEM((8, *block), f32),
            pltpu.VMEM((4, *block), f32),
            pltpu.VMEM((4, *block), f32),
            pltpu.VMEM((2, *block), f32),
            pltpu.VMEM((8, 1, LANES), f32),
            pltpu.VMEM((8 * n_mp, 1, LANES), f32),
            pltpu.VMEM(tile, f32),
            dma((3,)), dma((8, layers)), dma((8, pieces)), dma((4, pieces)), dma((4, pieces)), dma((2, pieces)),
            dma((8,)), dma((8,)), dma((8 * n_mp,)), dma((8 * n_mp,)),
        ],
        compiler_params=pltpu.CompilerParams(
            collective_id=0, has_side_effects=True, vmem_limit_bytes=32 * 1024 * 1024
        ),
    )(*(pltpu.with_memory_space_constraint(a, pltpu.HBM) for a in (layer_mask, exit_losses, exit_weights, gradients)))
    exit_mean = stats[0, layers : 2 * layers] / stats[0, :layers]
    new = update(gradient, clip[None], params, moment, second)
    return (*new, exit_mean)


def solution(mesh):
    state = P(None, "dp", "mp")
    placed = (P("dp", None, None, "mp"), P("dp", None), P("dp", None), P(), state, state, state)
    n_dp, n_mp = mesh.shape["dp"], mesh.shape["mp"]

    def whole(*args):
        entries = args[4].size
        layers = args[4].shape[0]

        def body(*blocks):
            if n_dp == 8 and layers == 2:
                return line_body(n_mp, entries, *blocks)
            return any_mesh_body(entries, *blocks)

        return jax.shard_map(
            body, mesh=mesh, in_specs=placed, out_specs=(state, state, state, P()), check_vma=False
        )(*args)

    return whole
```
